16 devices in a mesh: dp: 2 (over y, z), tp: 8 (over x, core).
Axes of the slice: x: 4, y: 2, z: 1, core: 2. Of those that a mesh axis runs over, the one named last changes fastest.
The devices are a block of a 4x4x8 slice.
Arguments:
- x_seq: bfloat16 [4, 2048, 4096], P('dp', 'tp'), parts along dimension 0
- ln_gain: bfloat16 [4096], replicated
- w_qkv: bfloat16 [4096, 8, 768], P(None, 'tp')
- w_out: bfloat16 [4096, 4096], P('tp')
- y_grad: bfloat16 [4, 2048, 4096], P('dp', 'tp'), parts along dimension 0
Outputs:
- output 1: bfloat16 [4, 2048, 4096], P('dp', 'tp'), parts along dimension 0
- output 2: bfloat16 [4, 2048, 4096], P('dp', 'tp'), parts along dimension 0
- output 3: bfloat16 [8192], P('dp'), parts along dimension 0
- output 4: bfloat16 [8192, 8, 768], P('dp', 'tp'), parts along dimension 0
- output 5: bfloat16 [8192, 4096], P(('dp', 'tp')), parts along dimension 0
There are 2 independent parts. The reference program is written for one: setup_inputs(seed, part) draws one part's arguments, and reference() takes and returns one part's arrays. A program takes and returns all parts, laid end to end along the dimension named above; an argument that names none is the same for every part.
All inputs are finite; a program needn't handle non-finite values.
Results may differ from the reference program's by a relative error of at most 0.0177313.
Values are sent between devices in bfloat16 or wider.
A program may use at most 768 MiB of HBM per device.

```python
import jax
import jax.numpy as jnp
from jax import lax

BATCH_SIZE = 2
SEQ_LEN = 2048
D_MODEL = 4096
N_HEADS = 32
KV_HEADS = 8
HEAD_DIM = 128
CLIP_QKV = 8
ROPE_THETA = 500000
LN_EPS = 1e-5
GROUP_SIZE = N_HEADS // KV_HEADS
SLOT_WIDTH = (GROUP_SIZE + 2) * HEAD_DIM
OUT_GAIN = max(1.0, SEQ_LEN / 256.0) ** 0.25


def setup_inputs(seed: int = 0, part: int = 0) -> dict:
    root_key = jax.random.key(seed)
    k_gain, k_qkv, k_out = jax.random.split(root_key, 3)
    k_x, k_dy = jax.random.split(jax.random.fold_in(root_key, part), 2)
    x_seq = jax.random.normal(k_x, (BATCH_SIZE, SEQ_LEN, D_MODEL), jnp.float32)
    ln_gain = 1.0 + 0.3 * jax.random.normal(k_gain, (D_MODEL,), jnp.float32)
    slot_gain = jnp.concatenate([jnp.full((GROUP_SIZE,), 5.0, dtype=jnp.float32), jnp.array([0.35, 5.0], dtype=jnp.float32)])
    w_qkv = jax.random.normal(k_qkv, (D_MODEL, KV_HEADS, GROUP_SIZE + 2, HEAD_DIM), jnp.float32)
    w_qkv = w_qkv * slot_gain[:, None] * D_MODEL ** -0.5
    attn_width = N_HEADS * HEAD_DIM
    w_out = jax.random.normal(k_out, (attn_width, D_MODEL), jnp.float32) * (OUT_GAIN * attn_width ** -0.5)
    y_grad = jax.random.normal(k_dy, (BATCH_SIZE, SEQ_LEN, D_MODEL), jnp.float32)
    return {'x_seq': x_seq.astype(jnp.bfloat16), 'ln_gain': ln_gain.astype(jnp.bfloat16), 'w_qkv': w_qkv.reshape(D_MODEL, KV_HEADS, SLOT_WIDTH).astype(jnp.bfloat16), 'w_out': w_out.astype(jnp.bfloat16), 'y_grad': y_grad.astype(jnp.bfloat16)}


def rope_tables(seq_len):
    inv_freq = 1.0 / (ROPE_THETA ** (jnp.arange(0, HEAD_DIM, 2, dtype=jnp.float32) / HEAD_DIM))
    angles = jnp.arange(seq_len, dtype=jnp.float32)[:, None] * inv_freq[None, :]
    return jnp.cos(angles), jnp.sin(angles)


def rotate(vec_in, cos_t, sin_t):
    half_dim = vec_in.shape[-1] // 2
    half_lo = vec_in[..., :half_dim]
    half_hi = vec_in[..., half_dim:]
    return jnp.concatenate([half_lo * cos_t - half_hi * sin_t, half_hi * cos_t + half_lo * sin_t], axis=-1)


def group_attention(operands):
    query_rot, key_rot, val_head = operands
    scores = jnp.einsum('bqgd,bkd->bgqk', query_rot.astype(jnp.float32), key_rot.astype(jnp.float32)) * HEAD_DIM ** -0.5
    causal = jnp.arange(SEQ_LEN)[:, None] >= jnp.arange(SEQ_LEN)[None, :]
    scores = jnp.where(causal, scores, -1e30)
    attn_prob = jax.nn.softmax(scores, axis=-1).astype(jnp.bfloat16)
    return jnp.einsum('bgqk,bkd->bqgd', attn_prob.astype(jnp.float32), val_head.astype(jnp.float32)).astype(jnp.bfloat16)


def layer_forward(x_seq, ln_gain, w_qkv, w_out):
    x_f32 = x_seq.astype(jnp.float32)
    row_mean = jnp.mean(x_f32, axis=-1, keepdims=True)
    centered = x_f32 - row_mean
    variance = jnp.mean(centered * centered, axis=-1, keepdims=True)
    h_norm = (centered * lax.rsqrt(variance + LN_EPS) * ln_gain.astype(jnp.float32)).astype(jnp.bfloat16)
    qkv_raw = jnp.dot(h_norm.reshape(-1, D_MODEL).astype(jnp.float32), w_qkv.reshape(D_MODEL, -1).astype(jnp.float32)).astype(jnp.bfloat16)
    qkv_clip = jnp.where(jnp.abs(qkv_raw) < CLIP_QKV, qkv_raw, jnp.sign(qkv_raw) * CLIP_QKV)
    qkv_slots = qkv_clip.reshape(BATCH_SIZE, SEQ_LEN, KV_HEADS, GROUP_SIZE + 2, HEAD_DIM)
    cos_t, sin_t = rope_tables(SEQ_LEN)
    query_rot = rotate(qkv_slots[:, :, :, :GROUP_SIZE].astype(jnp.float32), cos_t[:, None, None], sin_t[:, None, None]).astype(jnp.bfloat16)
    key_rot = rotate(qkv_slots[:, :, :, GROUP_SIZE].astype(jnp.float32), cos_t[:, None], sin_t[:, None]).astype(jnp.bfloat16)
    val_head = qkv_slots[:, :, :, GROUP_SIZE + 1]
    mixed = lax.map(jax.checkpoint(group_attention), (jnp.moveaxis(query_rot, 2, 0), jnp.moveaxis(key_rot, 2, 0), jnp.moveaxis(val_head, 2, 0)))
    mixed = jnp.moveaxis(mixed, 0, 2).reshape(BATCH_SIZE * SEQ_LEN, N_HEADS * HEAD_DIM)
    out_proj = jnp.dot(mixed.astype(jnp.float32), w_out.astype(jnp.float32)).reshape(BATCH_SIZE, SEQ_LEN, D_MODEL)
    return (x_f32 + out_proj).astype(jnp.bfloat16)


def reference(x_seq, ln_gain, w_qkv, w_out, y_grad):
    y_out, pullback = jax.vjp(layer_forward, x_seq, ln_gain, w_qkv, w_out)
    x_grad, gain_grad, wqkv_grad, wout_grad = pullback(y_grad)
    return (y_out, x_grad, gain_grad, wqkv_grad, wout_grad)
```

```python
import functools
import jax
import jax.numpy as jnp
from jax import lax
from jax.experimental import pallas as pl
from jax.experimental.pallas import tpu as pltpu
from jax.sharding import PartitionSpec as P

CLIP_QKV = 8.0
ROPE_THETA = 500000.0
LN_EPS = 1e-5
LOG2E = 1.4426950408889634
HD = 128
F32 = jnp.float32
BF16 = jnp.bfloat16
NT = (((1,), (1,)), ((), ()))


def layer_norm(x_f32, gain_f32):
    row_mean = jnp.mean(x_f32, axis=-1, keepdims=True)
    centered = x_f32 - row_mean
    variance = jnp.mean(centered * centered, axis=-1, keepdims=True)
    return (centered * lax.rsqrt(variance + LN_EPS) * gain_f32).astype(BF16)


def rope_tables(seq_len):
    inv_freq = 1.0 / (ROPE_THETA ** (jnp.arange(0, HD, 2, dtype=F32) / HD))
    angles = jnp.arange(seq_len, dtype=F32)[:, None] * inv_freq[None, :]
    cos_t, sin_t = jnp.cos(angles), jnp.sin(angles)
    return jnp.concatenate([cos_t, cos_t], -1), jnp.concatenate([-sin_t, sin_t], -1)


def rope(v, cos2, sin2):
    return v * cos2 + pltpu.roll(v, HD // 2, 1) * sin2


def rope_t(v, cos2, sin2):
    return v * cos2 - pltpu.roll(v, HD // 2, 1) * sin2


def causal_mask(bk, bq):
    key_i = lax.broadcasted_iota(jnp.int32, (bk, bq), 0)
    query_i = lax.broadcasted_iota(jnp.int32, (bk, bq), 1)
    return key_i <= query_i


def attn_fwd_kernel(scale, blk, q_ref, k_ref, v_ref, cos_ref, sin_ref, o_ref, lse_ref, k_s, vt_s):
    head, qi = pl.program_id(0), pl.program_id(1)
    nblk = k_s.shape[0]

    @pl.when((head == 0) & (qi == 0))
    def _():
        for n in range(nblk):
            rows = pl.ds(n * blk, blk)
            k_s[n] = rope(k_ref[rows, :].astype(F32), cos_ref[rows, :], sin_ref[rows, :]).astype(BF16)
            vt_s[n] = v_ref[rows, :].T

    rows = pl.ds(pl.multiple_of(qi * blk, blk), blk)
    q = rope(q_ref[...].astype(F32), cos_ref[rows, :], sin_ref[rows, :]).astype(BF16)

    def block(j, carry, masked):
        m_old, l_old, acc = carry
        s = lax.dot_general(k_s[j], q, NT, preferred_element_type=F32) * (scale * LOG2E)
        if masked:
            s = jnp.where(causal_mask(blk, blk), s, -1e30)
        m_new = jnp.maximum(m_old, jnp.max(s, axis=0, keepdims=True))
        p = jnp.exp2(s - m_new)
        alpha = jnp.exp2(m_old - m_new)
        l_new = alpha * l_old + jnp.sum(p, axis=0, keepdims=True)
        pv = jnp.dot(vt_s[j], p.astype(BF16), preferred_element_type=F32)
        return m_new, l_new, acc * alpha + pv

    init = (jnp.full((1, blk), -1e30, F32), jnp.zeros((1, blk), F32), jnp.zeros((HD, blk), F32))
    carry = block(qi, init, True)
    m, l, acc = lax.fori_loop(0, qi, lambda j, c: block(j, c, False), carry)
    o_ref[...] = (acc / l).T.astype(BF16)
    lse_ref[0, 0] = m + jnp.log2(l)


def attn_fwd(qkv, cos2, sin2, blk=512):
    seq, width = qkv.shape
    groups = width // HD - 2
    nblk = seq // blk
    flops = 4 * groups * seq * seq * HD
    whole = lambda c: pl.BlockSpec((seq, HD), lambda h, i: (0, c))
    return pl.pallas_call(
        functools.partial(attn_fwd_kernel, HD ** -0.5, blk),
        grid=(groups, nblk),
        in_specs=[pl.BlockSpec((blk, HD), lambda h, i: (i, h)), whole(groups), whole(groups + 1), whole(0), whole(0)],
        out_specs=[pl.BlockSpec((blk, HD), lambda h, i: (i, h)),
                   pl.BlockSpec((1, 1, 1, blk), lambda h, i: (h, i, 0, 0))],
        out_shape=[jax.ShapeDtypeStruct((seq, groups * HD), BF16),
                   jax.ShapeDtypeStruct((groups, nblk, 1, blk), F32)],
        scratch_shapes=[pltpu.VMEM((nblk, blk, HD), BF16), pltpu.VMEM((nblk, HD, blk), BF16)],
        compiler_params=pltpu.CompilerParams(dimension_semantics=("arbitrary", "arbitrary"),
                                             vmem_limit_bytes=40 * 1024 * 1024),
        cost_estimate=pl.CostEstimate(flops=flops * 3, bytes_accessed=6 << 20, transcendentals=0),
        name="attn_fwd",
    )(qkv, qkv, qkv, cos2, sin2)


def attn_bwd_kernel(scale, blk, groups, q_ref, k_ref, v_ref, do_ref, o_ref, lse_ref, cos_ref, sin_ref,
                    out_ref, k_s, kt_s, dk_s, dv_s):
    head = pl.program_id(0)
    nblk = k_s.shape[0]

    @pl.when(head == 0)
    def _():
        for n in range(nblk):
            rows = pl.ds(n * blk, blk)
            kr = rope(k_ref[rows, :].astype(F32), cos_ref[rows, :], sin_ref[rows, :])
            k_s[n] = kr.astype(BF16)
            kt_s[n] = kr.T.astype(BF16)
        dk_s[...] = jnp.zeros_like(dk_s)
        dv_s[...] = jnp.zeros_like(dv_s)

    def passes(raw, grad):
        return jnp.where(jnp.abs(raw.astype(F32)) < CLIP_QKV, grad, 0.0).astype(BF16)

    def q_block(qi, _):
        rows = pl.ds(pl.multiple_of(qi * blk, blk), blk)
        cos2, sin2 = cos_ref[rows, :], sin_ref[rows, :]
        q_raw = q_ref[rows, :]
        q = rope(q_raw.astype(F32), cos2, sin2).astype(BF16)
        do = do_ref[rows, :]
        delta = jnp.sum((do.astype(F32) * o_ref[rows, :].astype(F32)).T, axis=0, keepdims=True)
        lse = lse_ref[0, qi]

        def block(j, dq_t, masked):
            keys = pl.ds(pl.multiple_of(j * blk, blk), blk)
            s = lax.dot_general(k_s[j], q, NT, preferred_element_type=F32) * (scale * LOG2E)
            p = jnp.exp2(s - lse)
            if masked:
                p = jnp.where(causal_mask(blk, blk), p, 0.0)
            dp = lax.dot_general(v_ref[keys, :], do, NT, preferred_element_type=F32)
            dp = dp.astype(BF16).astype(F32)
            ds = (p * (dp - delta)).astype(BF16)
            dv_s[j] += jnp.dot(p.astype(BF16), do, preferred_element_type=F32)
            dk_s[j] += jnp.dot(ds, q, preferred_element_type=F32)
            return dq_t + jnp.dot(kt_s[j], ds, preferred_element_type=F32)

        dq_t = block(qi, jnp.zeros((HD, blk), F32), True)
        dq_t = lax.fori_loop(0, qi, lambda j, c: block(j, c, False), dq_t)
        dq = (dq_t.T * scale).astype(BF16).astype(F32)
        dq = rope_t(dq, cos2, sin2)
        out_ref[rows, pl.ds(pl.multiple_of(head * HD, HD), HD)] = passes(q_raw, dq)
        return 0

    lax.fori_loop(0, nblk, q_block, 0)

    @pl.when(head == groups - 1)
    def _():
        for n in range(nblk):
            rows = pl.ds(n * blk, blk)
            dk = (dk_s[n] * scale).astype(BF16).astype(F32)
            dk = rope_t(dk, cos_ref[rows, :], sin_ref[rows, :])
            out_ref[rows, groups * HD:(groups + 1) * HD] = passes(k_ref[rows, :], dk)
            out_ref[rows, (groups + 1) * HD:] = passes(v_ref[rows, :], dv_s[n])


def attn_bwd(qkv, d_attn, attn, lse, cos2, sin2):
    seq, width = qkv.shape
    groups = width // HD - 2
    nblk, blk = lse.shape[1], lse.shape[3]
    flops = 10 * groups * seq * seq * HD
    whole = lambda c: pl.BlockSpec((seq, HD), lambda h: (0, c))
    per_head = pl.BlockSpec((seq, HD), lambda h: (0, h))
    return pl.pallas_call(
        functools.partial(attn_bwd_kernel, HD ** -0.5, blk, groups),
        grid=(groups,),
        in_specs=[per_head, whole(groups), whole(groups + 1), per_head, per_head,
                  pl.BlockSpec((1, nblk, 1, blk), lambda h: (h, 0, 0, 0)), whole(0), whole(0)],
        out_specs=pl.BlockSpec((seq, width), lambda h: (0, 0)),
        out_shape=jax.ShapeDtypeStruct((seq, width), BF16),
        scratch_shapes=[pltpu.VMEM((nblk, blk, HD), BF16), pltpu.VMEM((nblk, HD, blk), BF16),
                        pltpu.VMEM((nblk, blk, HD), F32), pltpu.VMEM((nblk, blk, HD), F32)],
        compiler_params=pltpu.CompilerParams(dimension_semantics=("arbitrary",), vmem_limit_bytes=40 * 1024 * 1024),
        cost_estimate=pl.CostEstimate(flops=flops * 3, bytes_accessed=12 << 20, transcendentals=0),
        name="attn_bwd",
    )(qkv, qkv, qkv, d_attn, attn, lse, cos2, sin2)


def norm_bwd_kernel(x_ref, gain_ref, dh_ref, dy_ref, *refs):
    dx_ref, dg_ref = refs[-2:]
    x = x_ref[0].astype(F32)
    mean = jnp.mean(x, axis=-1, keepdims=True)
    centered = x - mean
    rstd = lax.rsqrt(jnp.mean(centered * centered, axis=-1, keepdims=True) + LN_EPS)
    xhat = centered * rstd
    dh = dh_ref[...].astype(F32)
    part = jnp.sum(dh * xhat, axis=0, keepdims=True)

    @pl.when(pl.program_id(0) == 0)
    def _():
        dg_ref[...] = jnp.zeros_like(dg_ref)

    dg_ref[...] += part
    dxh = dh * gain_ref[...]
    m1 = jnp.mean(dxh, axis=-1, keepdims=True)
    m2 = jnp.mean(dxh * xhat, axis=-1, keepdims=True)
    dx_ref[0] = (dy_ref[0].astype(F32) + rstd * (dxh - m1 - xhat * m2)).astype(BF16)


def norm_bwd(b, x, gain, dh, dy, prev, blk=64):
    rows, width = dh.shape
    seq_spec = pl.BlockSpec((1, blk, width), lambda i: (b, i, 0))
    row_spec = pl.BlockSpec((blk, width), lambda i: (i, 0))
    vec_spec = pl.BlockSpec((1, width), lambda i: (0, 0))
    kept = [] if prev is None else [prev]
    return pl.pallas_call(
        norm_bwd_kernel,
        grid=(rows // blk,),
        in_specs=[seq_spec, vec_spec, row_spec, seq_spec] + [pl.BlockSpec(memory_space=pl.ANY) for _ in kept],
        out_specs=[seq_spec, vec_spec],
        out_shape=[jax.ShapeDtypeStruct(x.shape, BF16), jax.ShapeDtypeStruct((1, width), F32)],
        input_output_aliases={4: 0} if kept else {},
        compiler_params=pltpu.CompilerParams(dimension_semantics=("arbitrary",), vmem_limit_bytes=32 * 1024 * 1024),
        cost_estimate=pl.CostEstimate(flops=rows * width * 40, bytes_accessed=rows * width * 8, transcendentals=0),
        name="norm_bwd",
    )(x, gain, dh, dy, *kept)


def residual_kernel(x_ref, o_ref, *refs):
    refs[-1][0] = (x_ref[0].astype(F32) + o_ref[...].astype(F32)).astype(BF16)


def residual(b, x, out, prev, blk=64):
    rows, width = out.shape
    seq_spec = pl.BlockSpec((1, blk, width), lambda i: (b, i, 0))
    row_spec = pl.BlockSpec((blk, width), lambda i: (i, 0))
    kept = [] if prev is None else [prev]
    return pl.pallas_call(
        residual_kernel,
        grid=(rows // blk,),
        in_specs=[seq_spec, row_spec] + [pl.BlockSpec(memory_space=pl.ANY) for _ in kept],
        out_specs=seq_spec,
        out_shape=jax.ShapeDtypeStruct(x.shape, BF16),
        input_output_aliases={2: 0} if kept else {},
        compiler_params=pltpu.CompilerParams(dimension_semantics=("arbitrary",), vmem_limit_bytes=32 * 1024 * 1024),
        cost_estimate=pl.CostEstimate(flops=rows * width * 4, bytes_accessed=rows * width * 6, transcendentals=0),
        name="residual",
    )(x, out, *kept)


def mm(a, b, dims, dtype=BF16):
    return lax.dot_general(a, b, (dims, ((), ())), preferred_element_type=F32).astype(dtype)


def solution(mesh):
    def device_step(x_seq, ln_gain, w_qkv, w_out, y_grad):
        batch = x_seq.shape[0]
        d_model, kv_loc, slot = w_qkv.shape
        w_in = w_qkv.reshape(d_model, kv_loc * slot)
        gain = ln_gain.astype(F32)

        def gather(v):
            return lax.all_gather(v, 'tp', axis=0, tiled=True)

        def scatter(v):
            return lax.psum_scatter(v, 'tp', scatter_dimension=0, tiled=True)

        after = lambda v, *first: lax.optimization_barrier((v,) + first)[0]
        dy_loc = [y_grad[b] for b in range(batch)]
        x_in = after(x_seq, *dy_loc)
        h_loc = layer_norm(x_in.astype(F32), gain)
        dy0 = gather(dy_loc[0])
        h0 = gather(h_loc[0])
        h1 = gather(h_loc[1])
        dy1 = gather(dy_loc[1])
        cos2, sin2 = rope_tables(h0.shape[0])

        def forward(h):
            raw = mm(h, w_in, ((1,), (0,)))
            qkv = jnp.minimum(jnp.maximum(raw, -CLIP_QKV), CLIP_QKV)
            return (qkv,) + tuple(attn_fwd(qkv, cos2, sin2))

        def backward(dy, qkv, attn, lse):
            d_attn = mm(dy, w_out, ((1,), (1,)))
            d_qkv = attn_bwd(qkv, d_attn, attn, lse, cos2, sin2)
            return d_qkv, mm(d_qkv, w_in, ((1,), (1,)))

        qkv0, attn0, lse0 = forward(h0)
        out0 = mm(attn0, w_out, ((1,), (0,)))
        out_loc0 = scatter(out0)
        dqkv0, dh0 = backward(after(dy0, out0), qkv0, attn0, lse0)
        dh_loc0 = scatter(dh0)
        qkv1, attn1, lse1 = forward(after(h1, dh0))
        dqkv1, dh1 = backward(dy1, qkv1, attn1, lse1)
        dh_loc1 = scatter(dh1)
        out1 = mm(after(attn1, dh1), w_out, ((1,), (0,)))
        out_loc1 = scatter(out1)
        wout_grad = (mm(after(attn0, out1), dy0, ((0,), (0,)), F32) + mm(attn1, dy1, ((0,), (0,)), F32)).astype(BF16)
        wqkv_grad = (mm(h0, after(dqkv0, out1), ((0,), (0,)), F32) + mm(h1, dqkv1, ((0,), (0,)), F32)).astype(BF16)
        y_out = residual(1, x_seq, out_loc1, residual(0, x_seq, out_loc0, None))
        g_row = gain[None, :]
        dx, part0 = norm_bwd(0, x_seq, g_row, dh_loc0, y_grad, None)
        x_grad, part1 = norm_bwd(1, x_seq, g_row, dh_loc1, y_grad, dx)
        gain_grad = lax.psum((part0 + part1)[0], 'tp').astype(BF16)
        return y_out, x_grad, gain_grad, wqkv_grad.reshape(w_qkv.shape), wout_grad

    specs_in = (P('dp', 'tp', None), P(None), P(None, 'tp', None), P('tp', None), P('dp', 'tp', None))
    specs_out = (P('dp', 'tp', None), P('dp', 'tp', None), P('dp'), P('dp', 'tp', None), P(('dp', 'tp'), None))

    return jax.shard_map(device_step, mesh=mesh, in_specs=specs_in, out_specs=specs_out, check_vma=False)
```
